256 devices in a mesh: replica: 64 (over z, y, core), model: 4 (over x).
Axes of the slice: x: 4, y: 4, z: 8, core: 2. Of those that a mesh axis runs over, the one named last changes fastest.
Arguments:
- partial_up: float32 [64, 1024, 4096], P('replica', None, 'model'), may hold values from -8 to 8
- partial_down: float32 [64, 4096, 1024], P('replica', 'model'), may hold values from -8 to 8
- partial_norm: float32 [64, 1024], P('replica'), may hold values from -16 to 16
- partial_bias: float32 [64, 1024], P('replica'), may hold values from -16 to 16
- master_up: float32 [1024, 4096], P('replica', 'model'), may hold values from -0.1875 to 0.1875
- master_down: float32 [4096, 1024], P('model', 'replica'), may hold values from -0.09375 to 0.09375
- master_norm: float32 [1024], P('replica'), may hold values from 0.25 to 1.75
- master_bias: float32 [1024], P('replica'), may hold values from -3 to 3
- memory_up: float32 [1024, 4096], P('replica', 'model'), may hold values from 0.05 to 0.8
- memory_down: float32 [4096, 1024], P('model', 'replica'), may hold values from 0.05 to 0.8
- memory_norm: float32 [1024], P('replica'), may hold values from 0.05 to 0.8
- memory_bias: float32 [1024], P('replica'), may hold values from 0.05 to 0.8
Outputs:
- compute_up: bfloat16 [1024, 4096], P(None, 'model')
- compute_down: bfloat16 [4096, 1024], P('model')
- compute_norm: bfloat16 [1024], replicated
- compute_bias: bfloat16 [1024], replicated
- stepped_up: float32 [1024, 4096], P('replica', 'model')
- stepped_down: float32 [4096, 1024], P('model', 'replica')
- stepped_norm: float32 [1024], P('replica')
- stepped_bias: float32 [1024], P('replica')
- state_new_up: float32 [1024, 4096], P('replica', 'model')
- state_new_down: float32 [4096, 1024], P('model', 'replica')
- state_new_norm: float32 [1024], P('replica')
- state_new_bias: float32 [1024], P('replica')
The draws below stay inside these ranges and needn't reach their ends.
All inputs are finite; a program needn't handle non-finite values.
Results may differ from the reference program's by a relative error of at most 0.001.
Values may be sent and summed in bfloat16 or wider, within the bound.
A program may use at most 128 MiB of HBM per device.

```python
import jax
import jax.numpy as jnp
from jax import lax

WIDTH = 1024
INNER = 4096
REPLICAS = 64


def spiked(result, key, source, target, parts, factor):
    owner, partner = [(jnp.arange(result.shape[dim]) // (result.shape[dim] // parts)).reshape([-1 if axis == dim else 1 for axis in range(result.ndim)]) for dim in (source, target)]
    chosen = jax.random.permutation(key, parts)[partner]
    strong = (owner == chosen) | (owner == (partner + parts // 2) % parts)
    return jnp.where(strong, factor * result, result)


def steps_of(own_key, extent, split, low, high):
    gain = 1.0
    for dim, shards_of in split:
        heights = jax.random.uniform(jax.random.fold_in(jax.random.fold_in(own_key, 6), dim), (shards_of,), jnp.float32, low / len(split), high / len(split))
        gain = gain * jnp.repeat(jnp.exp(heights), extent[dim] // shards_of).reshape((-1,) + (1,) * (len(extent) - 1 - dim))
    return gain


def bell_draw(own_key, extent, width, limit, shards=(), kind=jnp.bfloat16):
    factor_of = steps_of(own_key, extent, shards, -0.22, 0.18) if shards else 1.0
    array = jax.random.normal(own_key, extent, jnp.float32) * width * factor_of
    return jnp.minimum(jnp.maximum(array, -limit), limit).astype(kind)


def heavy_noise(rng, extent, width, reach, cuts, heavy, held_as=jnp.bfloat16):
    entries = width * jax.random.normal(rng, extent, jnp.float32)
    if cuts:
        entries = entries * steps_of(rng, extent, cuts, -0.22, 0.18)
    return jnp.clip(spiked(entries, jax.random.fold_in(rng, 3), *heavy), -reach, reach).astype(held_as)


def setup_inputs(seed: int = 0) -> dict:
    arg_keys = jax.random.split(jax.random.key(seed), 13)
    return {
        "partial_up": heavy_noise(arg_keys[0], (REPLICAS, WIDTH, INNER), 0.5, 8.0, ((0, 64), (2, 4)), (0, 1, 64, 4.0), jnp.float32),
        "partial_down": heavy_noise(arg_keys[1], (REPLICAS, INNER, WIDTH), 0.5, 8.0, ((0, 64), (1, 4)), (0, 2, 64, 4.0), jnp.float32),
        "partial_norm": heavy_noise(arg_keys[2], (REPLICAS, WIDTH), 1.0, 16.0, ((0, 64),), (0, 1, 64, 4.0), jnp.float32),
        "partial_bias": heavy_noise(arg_keys[3], (REPLICAS, WIDTH), 1.0, 16.0, ((0, 64),), (0, 1, 64, 4.0), jnp.float32),
        "master_up": bell_draw(arg_keys[4], (WIDTH, INNER), WIDTH ** -0.5, 0.1875, ((0, 64), (1, 4)), jnp.float32),
        "master_down": bell_draw(arg_keys[5], (INNER, WIDTH), INNER ** -0.5, 0.09375, ((0, 4), (1, 64)), jnp.float32),
        "master_norm": jnp.clip(1.0 + 0.15 * jax.random.normal(arg_keys[6], (WIDTH,), jnp.float32), 0.25, 1.75),
        "master_bias": bell_draw(arg_keys[7], (WIDTH,), 0.5, 3.0, ((0, 64),), jnp.float32),
        "memory_up": jnp.clip(0.05 + 0.75 * jax.random.uniform(arg_keys[8], (WIDTH, INNER), jnp.float32) ** steps_of(arg_keys[8], (WIDTH, INNER), ((0, 64), (1, 4)), -0.2, 0.2), 0.05, 0.8),
        "memory_down": jnp.clip(0.05 + 0.75 * jax.random.uniform(arg_keys[9], (INNER, WIDTH), jnp.float32) ** steps_of(arg_keys[9], (INNER, WIDTH), ((0, 4), (1, 64)), -0.2, 0.2), 0.05, 0.8),
        "memory_norm": jnp.clip(0.05 + 0.75 * jax.random.uniform(arg_keys[10], (WIDTH,), jnp.float32) ** steps_of(arg_keys[10], (WIDTH,), ((0, 64),), -0.2, 0.2), 0.05, 0.8),
        "memory_bias": jnp.clip(0.05 + 0.75 * jax.random.uniform(arg_keys[11], (WIDTH,), jnp.float32) ** steps_of(arg_keys[11], (WIDTH,), ((0, 64),), -0.2, 0.2), 0.05, 0.8),
    }


learn_rate = 0.05
hold_rate = 0.9

def reference(partial_up, partial_down, partial_norm, partial_bias, master_up, master_down, master_norm, master_bias, memory_up, memory_down, memory_norm, memory_bias):
    mean_up = lax.optimization_barrier(jnp.sum(partial_up.astype(jnp.float32), axis=0)) * REPLICAS ** (-0.5)
    mean_down = lax.optimization_barrier(jnp.sum(partial_down.astype(jnp.float32), axis=0)) * REPLICAS ** (-0.5)
    mean_norm = lax.optimization_barrier(jnp.sum(partial_norm.astype(jnp.float32), axis=0)) * REPLICAS ** (-0.5)
    mean_bias = lax.optimization_barrier(jnp.sum(partial_bias.astype(jnp.float32), axis=0)) * REPLICAS ** (-0.5)
    state_new_up = hold_rate * memory_up + (1.0 - hold_rate) * mean_up * mean_up
    stepped_up = master_up - learn_rate * mean_up * lax.rsqrt(state_new_up + 1e-06)
    state_new_down = hold_rate * memory_down + (1.0 - hold_rate) * mean_down * mean_down
    stepped_down = master_down - learn_rate * mean_down * lax.rsqrt(state_new_down + 1e-06)
    state_new_norm = hold_rate * memory_norm + (1.0 - hold_rate) * mean_norm * mean_norm
    stepped_norm = master_norm - learn_rate * mean_norm * lax.rsqrt(state_new_norm + 1e-06)
    state_new_bias = hold_rate * memory_bias + (1.0 - hold_rate) * mean_bias * mean_bias
    stepped_bias = master_bias - learn_rate * mean_bias * lax.rsqrt(state_new_bias + 1e-06)
    compute_up = stepped_up.astype(jnp.bfloat16)
    compute_down = stepped_down.astype(jnp.bfloat16)
    compute_norm = stepped_norm.astype(jnp.bfloat16)
    compute_bias = stepped_bias.astype(jnp.bfloat16)
    return (compute_up, compute_down, compute_norm, compute_bias, stepped_up, stepped_down, stepped_norm, stepped_bias, state_new_up, state_new_down, state_new_norm, state_new_bias)
```

```python
import jax
import jax.numpy as jnp
from jax import lax
from jax.experimental import pallas as pl
from jax.experimental.pallas import tpu as pltpu
from jax.sharding import PartitionSpec as P

learn_rate = 0.05
hold_rate = 0.9
NZ, NY = 8, 4
MEAN_RATE = 64 ** (-0.5)
WAYS = ((0, 1), (1, -1))
F32, BF16 = jnp.float32, jnp.bfloat16


def adapt(total, master, memory):
    mean = total * MEAN_RATE
    state = hold_rate * memory + (1.0 - hold_rate) * mean * mean
    return master - learn_rate * mean * lax.rsqrt(state + 1e-06), state


def slot_of(step, piece, half):
    if step == 1:
        return 0
    return 2 * step - (2 if piece == half else 3)


def kernel(
    up, dn, norm, bias, mu, md, mn, mb, su, sd, sn, sb,
    cu, cd, cn, cb, tu, td, tn, tb, nu, nd, nn, nb,
    own_up, peer_up, own_dn, peer_dn, vecs, peer_vec,
    in_y, in_z, in_z2, turned, in_yd, pair,
    ou, od, part_dn, tile_dn,
    v_mu, v_md, v_su, v_sd, v_mn, v_mb, v_sn, v_sb,
    o_tu, o_td, o_nu, o_nd, o_tn, o_tb, o_nn, o_nb, o_cn, o_cb,
    load_up, load_dn, load_small, pass_up, pass_dn, pass_vec, got_up, got_dn, got_vec,
    y_out, y_in, z_out, z_in, z2_out, z2_in, yd_out, yd_in, pair_out, pair_in,
    tile_out, tile_in, gz_out, gz_in, uz_out, uz_in, uy_out, uy_in, uf_out, uf_in,
    dpass, dgot, upass, ugot, store_sem,
):
    me = lax.axis_index("replica")
    core = lax.rem(me, 2)
    row = lax.rem(me // 2, NY)
    lay = me // (2 * NY)
    other = 1 - core

    def place(z, y, c):
        return {"replica": (z * NY + y) * 2 + c}

    def zed(k):
        return lax.rem(lay + k + 2 * NZ, NZ)

    def why(k):
        return lax.rem(row + k + 2 * NY, NY)

    peer = place(lay, row, other)
    z_next = [place(zed(way), row, core) for _, way in WAYS]
    y_next = [place(lay, why(way), core) for _, way in WAYS]

    def remote(src, dst, out, arrive, where):
        return pltpu.make_async_remote_copy(
            src_ref=src, dst_ref=dst, send_sem=out, recv_sem=arrive,
            device_id=where, device_id_type=pl.DeviceIdType.MESH,
        )

    sent = []

    def go(copy):
        copy.start()
        sent.append(copy)
        return copy

    smalls = [
        (norm, vecs.at[0]), (bias, vecs.at[1]), (mu, v_mu), (md, v_md), (su, v_su), (sd, v_sd),
        (mn, v_mn), (mb, v_mb), (sn, v_sn), (sb, v_sb),
    ]
    small_copies = [
        pltpu.make_async_copy(a, b, load_small.at[i]) for i, (a, b) in enumerate(smalls)
    ]
    for c in small_copies:
        c.start()

    def up_piece(ky, p, c):
        return up.at[pl.ds(4 * p, 4), why(ky), c]

    def dn_piece(k, p, c):
        rows = pl.multiple_of(c * 512 + p * 256, 256)
        return dn.at[pl.ds(rows, 256), pl.ds(pl.multiple_of(zed(k) * 128, 128), 128)]

    dn_order = [(4, 0), (4, 1), (3, 1), (5, 0), (3, 0), (5, 1), (2, 0), (2, 1), (6, 0), (6, 1), (1, 0), (1, 1), (7, 0), (7, 1), (0, 0), (0, 1)]
    up_order = [(2, 0), (2, 1), (1, 1), (3, 0), (1, 0), (3, 1), (0, 0), (0, 1)]
    order = []
    for i in range(8):
        order += [("d",) + dn_order[2 * i], ("d",) + dn_order[2 * i + 1], ("u",) + up_order[i]]
    order = [("d", 4, 0), ("d", 4, 1), ("u", 2, 0), ("u", 2, 1), ("d", 3, 1), ("d", 5, 0), ("u", 1, 1), ("u", 3, 0)] + [
        o for o in order if o not in (("d", 4, 0), ("d", 4, 1), ("u", 2, 0), ("u", 2, 1), ("d", 3, 1), ("d", 5, 0), ("u", 1, 1), ("u", 3, 0))
    ]
    loads, passes = {}, {}
    for kind, k, p in order:
        if kind == "u":
            loads[kind, k, p] = pltpu.make_async_copy(
                up_piece(k, p, core), own_up.at[k, pl.ds(4 * p, 4)], load_up.at[k, p]
            )
            passes[kind, k, p] = remote(
                up_piece(k, p, other), peer_up.at[k, pl.ds(4 * p, 4)],
                pass_up.at[k, p], got_up.at[k, p], peer,
            )
        else:
            loads[kind, k, p] = pltpu.make_async_copy(
                dn_piece(k, p, core), own_dn.at[k, p, pl.ds(0, 256)], load_dn.at[k, p]
            )
            passes[kind, k, p] = remote(
                dn_piece(k, p, other), peer_dn.at[k, p], pass_dn.at[k, p], got_dn.at[k, p], peer
            )

    barrier = pltpu.get_barrier_semaphore()
    friends = [peer] + z_next
    for ky in (1, 2, 3):
        friends += [place(lay, why(ky), core), place(lay, why(ky), other)]
    for friend in friends:
        pl.semaphore_signal(barrier, inc=1, device_id=friend, device_id_type=pl.DeviceIdType.MESH)
    for key in order:
        loads[key].start()
    pl.semaphore_wait(barrier, len(friends))
    small_copies[0].wait()
    small_copies[1].wait()
    vec_pass = go(remote(vecs.at[other], peer_vec, pass_vec, got_vec, peer))
    for key in order:
        go(passes[key])

    vec_pass.wait_recv()
    peer_vec[...] = vecs[core] + peer_vec[...]

    def join(kind, k, p):
        loads[kind, k, p].wait()
        passes[kind, k, p].wait_recv()
        if kind == "u":
            own_up[k, 4 * p : 4 * p + 4] += peer_up[k, 4 * p : 4 * p + 4]
        else:
            own_dn[k, p, 0:256] += peer_dn[k, p]
            line = peer_vec[:, pl.ds(pl.multiple_of(zed(k) * 128, 128), 128)]
            own_dn[k, p, 256:264] = jnp.broadcast_to(line, (8, 128))

    def reducer(count, mine, arrive, out, inn, neighbour):
        reach = count // 2

        def chunk(way, step):
            return (way * (reach + 1 - step)) % count

        def send(way, step, piece):
            di, direction = way
            slot = slot_of(step, piece, di)
            go(remote(
                mine(chunk(direction, step), piece), arrive.at[di, slot],
                out.at[di, slot], inn.at[di, slot], neighbour[di],
            ))

        def take(way, step, piece):
            di, direction = way
            slot = slot_of(step, piece, di)
            remote(
                mine(chunk(direction, step), piece), arrive.at[di, slot],
                out.at[di, slot], inn.at[di, slot], neighbour[di],
            ).wait_recv()
            ref = mine(chunk(direction, step + 1), piece)
            ref[...] += arrive[di, slot]
            if step < reach:
                send(way, step + 1, piece)

        return send, take

    z_send, z_take = reducer(NZ, lambda k, p: own_dn.at[k, p], in_z, z_out, z_in, z_next)
    y_send, y_take = reducer(
        NY, lambda k, p: own_up.at[k, pl.ds(4 * p, 4)], in_y, y_out, y_in, y_next
    )
    z2_send, z2_take = reducer(
        NZ, lambda k, p: own_up.at[0, zed(k), pl.ds(8 * p, 8)], in_z2, z2_out, z2_in, z_next
    )
    yd_send, yd_take = reducer(
        NY,
        lambda k, p: turned.at[pl.ds(pl.multiple_of(16 * (2 * why(k) + p), 16), 16)],
        in_yd, yd_out, yd_in, y_next,
    )

    def both(act, step, near):
        for way in WAYS:
            act(way, step, way[0] if near else 1 - way[0])

    for p in (0, 1):
        join("d", 4, p)
    both(z_send, 1, True)
    for p in (0, 1):
        join("u", 2, p)
    both(y_send, 1, True)
    join("d", 3, 1)
    join("d", 5, 0)
    both(z_send, 2, False)
    join("u", 1, 1)
    join("u", 3, 0)
    both(y_send, 2, False)
    for key in order[8:]:
        if key[1] != 0:
            join(*key)
    both(z_take, 1, True)
    for key in order[8:]:
        if key[1] == 0:
            join(*key)
    both(y_take, 1, True)
    both(z_take, 2, False)
    both(z_take, 2, True)
    both(z_take, 3, False)
    both(y_take, 2, False)
    both(z_take, 3, True)
    both(y_take, 2, True)
    both(z2_send, 1, True)
    both(z2_send, 2, False)
    both(z_take, 4, False)
    both(z2_take, 1, True)
    both(z_take, 4, True)

    for p in (0, 1):
        turned[:, 256 * p : 256 * p + 256] = own_dn[0, p, 0:256].T
    turned[:, 512:640] = own_dn[0, 0, 136:264].T
    both(yd_send, 1, True)
    both(yd_send, 2, False)
    both(z2_take, 2, False)
    both(z2_take, 2, True)
    both(yd_take, 1, True)
    both(z2_take, 3, False)
    both(yd_take, 2, False)
    both(z2_take, 3, True)
    both(yd_take, 2, True)

    def mine_at(c):
        return pl.ds(pl.multiple_of(16 * (2 * row + c), 16), 16)

    pair_pass = go(remote(turned.at[mine_at(other)], pair.at[core], pair_out, pair_in, peer))
    pair[core] = turned[mine_at(core), :]
    for c in small_copies[2:]:
        c.wait()
    pair_pass.wait_recv()

    stores = []

    def keep(src, dst):
        copy = pltpu.make_async_copy(src, dst, store_sem.at[len(stores)])
        copy.start()
        stores.append(copy)

    lines = ((v_mn, v_sn, o_tn, o_nn, o_cn, cn, tn, nn), (v_mb, v_sb, o_tb, o_nb, o_cb, cb, tb, nb))
    for r in (0, 1):
        cols = slice(512 * r, 512 * r + 512)
        stepped, state = adapt(pair[r, :, 0:512], v_md[:, cols], v_sd[:, cols])
        o_td[:, cols] = stepped
        o_nd[:, cols] = state
        part_dn[r, :, 0:512] = stepped.astype(BF16)
        block = jnp.concatenate([pair[r, :, 512:640], jnp.zeros((112, 128), F32)], axis=0).T
        master, memory, o_t, o_n = lines[r][:4]
        stepped, state = adapt(block[127:128, 0:16], master[...], memory[...])
        o_t[...] = stepped
        o_n[...] = state
        wide = jnp.concatenate([stepped, jnp.zeros((1, 112), F32)], axis=1)
        part_dn[r, :, 512:640] = jnp.broadcast_to(wide, (128, 128)).T[0:16].astype(BF16)

    tile_copies = []
    for ky in range(NY):
        for x in (0, 1):
            if ky == 0 and x == 0:
                continue
            c = core if x == 0 else other
            tile_copies.append(go(remote(
                part_dn.at[c], tile_dn.at[2 * row + core], tile_out.at[ky, x], tile_in.at[ky, x],
                place(lay, why(ky), c),
            )))
    tile_dn[2 * row + core] = part_dn[core]
    both(z2_take, 4, False)
    both(z2_take, 4, True)
    stepped, state = adapt(own_up[0, lay], v_mu[...], v_su[...])
    o_tu[...] = stepped
    o_nu[...] = state
    ou[lay, row, core] = stepped.astype(BF16)

    def spread_up(way, step, piece):
        di, direction = way
        ref = ou.at[zed(-direction * (step - 1)), row, core, :, pl.ds(512 * piece, 512)]
        slot = 2 * step - (2 if piece == di else 1)
        return remote(ref, ref, uz_out.at[di, slot], uz_in.at[di, slot], z_next[di])

    def spread_dn(way, step, piece):
        di, direction = way
        rows = pl.ds(0, 256) if piece == 0 else pl.ds(256, 272)
        ref = od.at[zed(-direction * (step - 1)), core, rows]
        slot = 2 * step - (2 if piece == di else 1)
        return remote(ref, ref, gz_out.at[di, slot], gz_in.at[di, slot], z_next[di])

    def aside(di, kz):
        ref = ou.at[zed(kz), row, core]
        return remote(ref, ref, uy_out.at[di, kz % NZ], uy_in.at[di, kz % NZ], y_next[di])

    def aside_far(way, kz):
        di, direction = way
        ref = ou.at[zed(kz), why(-direction), core, :, pl.ds(512 * di, 512)]
        return remote(ref, ref, uf_out.at[di, kz % NZ], uf_in.at[di, kz % NZ], y_next[di])

    def across_dn(k):
        ref = od.at[zed(k), core]
        return remote(ref, ref, dpass.at[k % NZ], dgot.at[k % NZ], peer)

    def across_up(ky):
        ref = ou.at[:, why(ky), core]
        return remote(ref, ref, upass.at[ky], ugot.at[ky], peer)

    for way in WAYS:
        go(spread_up(way, 1, way[0]))
        go(spread_up(way, 1, 1 - way[0]))
    for di in (0, 1):
        go(aside(di, 0))

    for copy in tile_copies:
        copy.wait_recv()
    for j in range(5):
        flat = tile_dn[:, :, 128 * j : 128 * j + 128].astype(F32).reshape(128, 128).T.astype(BF16)
        if j < 4:
            od[lay, core, 128 * j : 128 * j + 128] = flat
        else:
            od[lay, core, 512:528] = flat[112:128]
    for way in WAYS:
        go(spread_dn(way, 1, way[0]))
        go(spread_dn(way, 1, 1 - way[0]))
    go(across_dn(0))

    def onward(spread, step):
        for near in (True, False):
            if step == 4 and not near:
                continue
            for way in WAYS:
                piece = way[0] if near else 1 - way[0]
                spread(way, step, piece).wait_recv()
                if step < 3 or (step == 3 and near):
                    go(spread(way, step + 1, piece))

    far = []
    for step in (1, 2, 3, 4):
        onward(spread_up, step)
        for kz in (step, -step) if step < 4 else (4,):
            for di in (0, 1):
                go(aside(di, kz))
        onward(spread_dn, step)
        for k in (step, -step) if step < 4 else (4,):
            go(across_dn(k))
        for kz in (step - 1, 1 - step) if step > 1 else (0,):
            for way in WAYS:
                aside(way[0], kz).wait_recv()
                far.append(go(aside_far(way, kz)))
    go(across_up(0))
    for kz in (4,):
        for way in WAYS:
            aside(way[0], kz).wait_recv()
            far.append(go(aside_far(way, kz)))
    go(across_up(1))
    go(across_up(3))
    for copy in far:
        copy.wait_recv()
    go(across_up(2))

    def keep_up(y, c):
        keep(ou.at[:, y, c], cu.at[:, y, c])

    def keep_dn(z, r):
        keep(
            od.at[z, r, pl.ds(0, 512)],
            cd.at[pl.ds(pl.multiple_of(512 * r, 512), 512), pl.ds(pl.multiple_of(128 * z, 128), 128)],
        )

    for a, b in ((o_tu, tu), (o_td, td), (o_nu, nu), (o_nd, nd), (o_tn, tn), (o_tb, tb), (o_nn, nn), (o_nb, nb)):
        keep(a, b)
    for ky in range(NY):
        keep_up(why(ky), core)
    for k in range(NZ):
        keep_dn(zed(k), core)
    for k in range(NZ):
        across_dn(k).wait_recv()
        keep_dn(zed(k), other)
    for z in range(NZ):
        o_cn[:, 128 * z : 128 * z + 128] = od[z, 0, 527:528]
        o_cb[:, 128 * z : 128 * z + 128] = od[z, 1, 527:528]
    keep(o_cn, cn)
    keep(o_cb, cb)
    for ky in (0, 1, 3, 2):
        across_up(ky).wait_recv()
        keep_up(why(ky), other)
    for copy in sent:
        copy.wait_send()
    for copy in stores:
        copy.wait()


def on_device(
    partial_up, partial_down, partial_norm, partial_bias,
    master_up, master_down, master_norm, master_bias,
    memory_up, memory_down, memory_norm, memory_bias,
):
    def shape(s, t=F32):
        return jax.ShapeDtypeStruct(s, t)

    def vm(*s, t=F32):
        return pltpu.VMEM(s, t)

    dma = pltpu.SemaphoreType.DMA
    anyw = pl.BlockSpec(memory_space=pl.ANY)
    out = pl.pallas_call(
        kernel,
        out_shape=(
            shape((NZ, NY, 2, 16, 1024), BF16), shape((1024, 1024), BF16),
            shape((1, 1024), BF16), shape((1, 1024), BF16),
            shape((16, 1024)), shape((16, 1024)), shape((1, 16)), shape((1, 16)),
            shape((16, 1024)), shape((16, 1024)), shape((1, 16)), shape((1, 16)),
        ),
        in_specs=[anyw] * 12,
        out_specs=(anyw,) * 12,
        scratch_shapes=[
            vm(NY, NZ, 16, 1024), vm(NY, NZ, 16, 1024),
            vm(NZ, 2, 264, 128), vm(NZ, 2, 256, 128), vm(2, 1, 1024), vm(1, 1024),
            vm(2, 3, 4, 16, 1024), vm(2, 7, 264, 128), vm(2, 7, 8, 1024),
            vm(128, 640), vm(2, 3, 16, 640), vm(2, 16, 640),
            vm(NZ, NY, 2, 16, 1024, t=BF16), vm(NZ, 2, 528, 128, t=BF16),
            vm(2, 16, 640, t=BF16), vm(8, 16, 640, t=BF16),
            vm(16, 1024), vm(16, 1024), vm(16, 1024), vm(16, 1024),
            vm(1, 16), vm(1, 16), vm(1, 16), vm(1, 16),
            vm(16, 1024), vm(16, 1024), vm(16, 1024), vm(16, 1024),
            vm(1, 16), vm(1, 16), vm(1, 16), vm(1, 16),
            vm(1, 1024, t=BF16), vm(1, 1024, t=BF16),
            dma((NY, 2)), dma((NZ, 2)), dma((10,)), dma((NY, 2)), dma((NZ, 2)), dma,
            dma((NY, 2)), dma((NZ, 2)), dma,
            dma((2, 3)), dma((2, 3)), dma((2, 7)), dma((2, 7)), dma((2, 7)), dma((2, 7)),
            dma((2, 3)), dma((2, 3)), dma, dma,
            dma((NY, 2)), dma((NY, 2)), dma((2, 7)), dma((2, 7)), dma((2, 7)), dma((2, 7)),
            dma((2, NZ)), dma((2, NZ)), dma((2, NZ)), dma((2, NZ)),
            dma((NZ,)), dma((NZ,)), dma((NY,)), dma((NY,)), dma((34,)),
        ],
        compiler_params=pltpu.CompilerParams(collective_id=0, has_side_effects=True),
        name="reduce_step_gather",
    )(
        partial_up.reshape(NZ, NY, 2, 16, 1024), partial_down[0], partial_norm, partial_bias,
        master_up, master_down.T, master_norm[None], master_bias[None],
        memory_up, memory_down.T, memory_norm[None], memory_bias[None],
    )
    cu, cd, cn, cb, tu, td, tn, tb, nu, nd, nn, nb = out
    return (
        cu.reshape(1024, 1024), cd, cn[0], cb[0],
        tu, td.T, tn[0], tb[0], nu, nd.T, nn[0], nb[0],
    )


def solution(mesh):
    in_specs = (
        P("replica", None, "model"), P("replica", "model", None), P("replica", None), P("replica", None),
        P("replica", "model"), P("model", "replica"), P("replica"), P("replica"),
        P("replica", "model"), P("model", "replica"), P("replica"), P("replica"),
    )
    out_specs = (
        P(None, "model"), P("model", None), P(), P(),
        P("replica", "model"), P("model", "replica"), P("replica"), P("replica"),
        P("replica", "model"), P("model", "replica"), P("replica"), P("replica"),
    )
    return jax.shard_map(
        on_device, mesh=mesh, in_specs=in_specs, out_specs=out_specs, check_vma=False
    )
```

```python
import jax
import jax.numpy as jnp
from jax import lax
from jax.experimental import pallas as pl
from jax.experimental.pallas import tpu as pltpu
from jax.sharding import PartitionSpec as P

learn_rate = 0.05
hold_rate = 0.9
NZ, NY = 8, 4
MEAN_RATE = 64 ** (-0.5)
WAYS = ((0, 1), (1, -1))
F32, BF16 = jnp.float32, jnp.bfloat16


def adapt(total, master, memory):
    mean = total * MEAN_RATE
    state = hold_rate * memory + (1.0 - hold_rate) * mean * mean
    return master - learn_rate * mean * lax.rsqrt(state + 1e-06), state


def slot_of(step, piece, half):
    if step == 1:
        return 0
    return 2 * step - (2 if piece == half else 3)


def kernel(
    up, dn, norm, bias, mu, md, mn, mb, su, sd, sn, sb,
    ou, od, o_tu, o_td, o_nu, o_nd, o_tn, o_tb, o_nn, o_nb,
    own_up, peer_up, own_dn, peer_dn, vecs, peer_vec,
    in_y, in_z, in_z2, turned, in_yd, pair,
    part_dn, tile_dn,
    v_mu, v_md, v_su, v_sd, v_mn, v_mb, v_sn, v_sb,
    load_up, load_dn, load_small, pass_up, pass_dn, pass_vec, got_up, got_dn, got_vec,
    y_out, y_in, z_out, z_in, z2_out, z2_in, yd_out, yd_in, pair_out, pair_in,
    tile_out, tile_in, gz_out, gz_in, uz_out, uz_in, uy_out, uy_in, uf_out, uf_in,
    dpass, dgot, upass, ugot,
):
    me = lax.axis_index("replica")
    core = lax.rem(me, 2)
    row = lax.rem(me // 2, NY)
    lay = me // (2 * NY)
    other = 1 - core

    def place(z, y, c):
        return {"replica": (z * NY + y) * 2 + c}

    def zed(k):
        return lax.rem(lay + k + 2 * NZ, NZ)

    def why(k):
        return lax.rem(row + k + 2 * NY, NY)

    peer = place(lay, row, other)
    z_next = [place(zed(way), row, core) for _, way in WAYS]
    y_next = [place(lay, why(way), core) for _, way in WAYS]

    def remote(src, dst, out, arrive, where):
        return pltpu.make_async_remote_copy(
            src_ref=src, dst_ref=dst, send_sem=out, recv_sem=arrive,
            device_id=where, device_id_type=pl.DeviceIdType.MESH,
        )

    sent = []

    def go(copy):
        copy.start()
        sent.append(copy)
        return copy

    smalls = [
        (norm, vecs.at[0]), (bias, vecs.at[1]), (mu, v_mu), (md, v_md), (su, v_su), (sd, v_sd),
        (mn, v_mn), (mb, v_mb), (sn, v_sn), (sb, v_sb),
    ]
    small_copies = [
        pltpu.make_async_copy(a, b, load_small.at[i]) for i, (a, b) in enumerate(smalls)
    ]
    for c in small_copies:
        c.start()

    def up_piece(ky, p, c):
        return up.at[pl.ds(4 * p, 4), why(ky), c]

    def dn_piece(k, p, c):
        rows = pl.multiple_of(c * 512 + p * 256, 256)
        return dn.at[pl.ds(rows, 256), pl.ds(pl.multiple_of(zed(k) * 128, 128), 128)]

    dn_order = [(4, 0), (4, 1), (3, 1), (5, 0), (3, 0), (5, 1), (2, 0), (2, 1), (6, 0), (6, 1), (1, 0), (1, 1), (7, 0), (7, 1), (0, 0), (0, 1)]
    up_order = [(2, 0), (2, 1), (1, 1), (3, 0), (1, 0), (3, 1), (0, 0), (0, 1)]
    order = []
    for i in range(8):
        order += [("d",) + dn_order[2 * i], ("d",) + dn_order[2 * i + 1], ("u",) + up_order[i]]
    order = [("d", 4, 0), ("d", 4, 1), ("u", 2, 0), ("u", 2, 1), ("d", 3, 1), ("d", 5, 0), ("u", 1, 1), ("u", 3, 0)] + [
        o for o in order if o not in (("d", 4, 0), ("d", 4, 1), ("u", 2, 0), ("u", 2, 1), ("d", 3, 1), ("d", 5, 0), ("u", 1, 1), ("u", 3, 0))
    ]
    loads, passes = {}, {}
    for kind, k, p in order:
        if kind == "u":
            loads[kind, k, p] = pltpu.make_async_copy(
                up_piece(k, p, core), own_up.at[k, pl.ds(4 * p, 4)], load_up.at[k, p]
            )
            passes[kind, k, p] = remote(
                up_piece(k, p, other), peer_up.at[k, pl.ds(4 * p, 4)],
                pass_up.at[k, p], got_up.at[k, p], peer,
            )
        else:
            loads[kind, k, p] = pltpu.make_async_copy(
                dn_piece(k, p, core), own_dn.at[k, p, pl.ds(0, 256)], load_dn.at[k, p]
            )
            passes[kind, k, p] = remote(
                dn_piece(k, p, other), peer_dn.at[k, p], pass_dn.at[k, p], got_dn.at[k, p], peer
            )

    barrier = pltpu.get_barrier_semaphore()
    friends = [peer] + z_next
    for ky in (1, 2, 3):
        friends += [place(lay, why(ky), core), place(lay, why(ky), other)]
    for friend in friends:
        pl.semaphore_signal(barrier, inc=1, device_id=friend, device_id_type=pl.DeviceIdType.MESH)
    for key in order:
        loads[key].start()
    pl.semaphore_wait(barrier, len(friends))
    small_copies[0].wait()
    small_copies[1].wait()
    vec_pass = go(remote(vecs.at[other], peer_vec, pass_vec, got_vec, peer))
    for key in order:
        go(passes[key])

    vec_pass.wait_recv()
    peer_vec[...] = vecs[core] + peer_vec[...]

    def join(kind, k, p):
        loads[kind, k, p].wait()
        passes[kind, k, p].wait_recv()
        if kind == "u":
            own_up[k, 4 * p : 4 * p + 4] += peer_up[k, 4 * p : 4 * p + 4]
        else:
            own_dn[k, p, 0:256] += peer_dn[k, p]
            line = peer_vec[:, pl.ds(pl.multiple_of(zed(k) * 128, 128), 128)]
            own_dn[k, p, 256:264] = jnp.broadcast_to(line, (8, 128))

    def reducer(count, mine, arrive, out, inn, neighbour):
        reach = count // 2

        def chunk(way, step):
            return (way * (reach + 1 - step)) % count

        def send(way, step, piece):
            di, direction = way
            slot = slot_of(step, piece, di)
            go(remote(
                mine(chunk(direction, step), piece), arrive.at[di, slot],
                out.at[di, slot], inn.at[di, slot], neighbour[di],
            ))

        def take(way, step, piece):
            di, direction = way
            slot = slot_of(step, piece, di)
            remote(
                mine(chunk(direction, step), piece), arrive.at[di, slot],
                out.at[di, slot], inn.at[di, slot], neighbour[di],
            ).wait_recv()
            ref = mine(chunk(direction, step + 1), piece)
            ref[...] += arrive[di, slot]
            if step < reach:
                send(way, step + 1, piece)

        return send, take

    z_send, z_take = reducer(NZ, lambda k, p: own_dn.at[k, p], in_z, z_out, z_in, z_next)
    y_send, y_take = reducer(
        NY, lambda k, p: own_up.at[k, pl.ds(4 * p, 4)], in_y, y_out, y_in, y_next
    )
    z2_send, z2_take = reducer(
        NZ, lambda k, p: own_up.at[0, zed(k), pl.ds(8 * p, 8)], in_z2, z2_out, z2_in, z_next
    )
    yd_send, yd_take = reducer(
        NY,
        lambda k, p: turned.at[pl.ds(pl.multiple_of(16 * (2 * why(k) + p), 16), 16)],
        in_yd, yd_out, yd_in, y_next,
    )

    def both(act, step, near):
        for way in WAYS:
            act(way, step, way[0] if near else 1 - way[0])

    for p in (0, 1):
        join("d", 4, p)
    both(z_send, 1, True)
    for p in (0, 1):
        join("u", 2, p)
    both(y_send, 1, True)
    join("d", 3, 1)
    join("d", 5, 0)
    both(z_send, 2, False)
    join("u", 1, 1)
    join("u", 3, 0)
    both(y_send, 2, False)
    for key in order[8:]:
        if key[1] != 0:
            join(*key)
    both(z_take, 1, True)
    for key in order[8:]:
        if key[1] == 0:
            join(*key)
    both(y_take, 1, True)
    both(z_take, 2, False)
    both(z_take, 2, True)
    both(z_take, 3, False)
    both(y_take, 2, False)
    both(z_take, 3, True)
    both(y_take, 2, True)
    both(z2_send, 1, True)
    both(z2_send, 2, False)
    both(z_take, 4, False)
    both(z2_take, 1, True)
    both(z_take, 4, True)

    for p in (0, 1):
        turned[:, 256 * p : 256 * p + 256] = own_dn[0, p, 0:256].T
    turned[:, 512:640] = own_dn[0, 0, 136:264].T
    both(yd_send, 1, True)
    both(yd_send, 2, False)
    both(z2_take, 2, False)
    both(z2_take, 2, True)
    both(yd_take, 1, True)
    both(z2_take, 3, False)
    both(yd_take, 2, False)
    both(z2_take, 3, True)
    both(yd_take, 2, True)

    def mine_at(c):
        return pl.ds(pl.multiple_of(16 * (2 * row + c), 16), 16)

    pair_pass = go(remote(turned.at[mine_at(other)], pair.at[core], pair_out, pair_in, peer))
    pair[core] = turned[mine_at(core), :]
    for c in small_copies[2:]:
        c.wait()
    pair_pass.wait_recv()

    lines = ((v_mn, v_sn, o_tn, o_nn), (v_mb, v_sb, o_tb, o_nb))
    for r in (0, 1):
        cols = slice(512 * r, 512 * r + 512)
        stepped, state = adapt(pair[r, :, 0:512], v_md[:, cols], v_sd[:, cols])
        o_td[:, cols] = stepped
        o_nd[:, cols] = state
        part_dn[r, :, 0:512] = stepped.astype(BF16)
        block = jnp.concatenate([pair[r, :, 512:640], jnp.zeros((112, 128), F32)], axis=0).T
        master, memory, o_t, o_n = lines[r]
        stepped, state = adapt(block[127:128, 0:16], master[...], memory[...])
        o_t[...] = stepped
        o_n[...] = state
        wide = jnp.concatenate([stepped, jnp.zeros((1, 112), F32)], axis=1)
        part_dn[r, :, 512:640] = jnp.broadcast_to(wide, (128, 128)).T[0:16].astype(BF16)

    tile_copies = []
    for ky in range(NY):
        for x in (0, 1):
            if ky == 0 and x == 0:
                continue
            c = core if x == 0 else other
            tile_copies.append(go(remote(
                part_dn.at[c], tile_dn.at[2 * row + core], tile_out.at[ky, x], tile_in.at[ky, x],
                place(lay, why(ky), c),
            )))
    tile_dn[2 * row + core] = part_dn[core]
    both(z2_take, 4, False)
    both(z2_take, 4, True)
    stepped, state = adapt(own_up[0, lay], v_mu[...], v_su[...])
    o_tu[...] = stepped
    o_nu[...] = state
    ou[lay, row, core] = stepped.astype(BF16)

    def spread_up(way, step, piece):
        di, direction = way
        ref = ou.at[zed(-direction * (step - 1)), row, core, :, pl.ds(512 * piece, 512)]
        slot = 2 * step - (2 if piece == di else 1)
        return remote(ref, ref, uz_out.at[di, slot], uz_in.at[di, slot], z_next[di])

    def spread_dn(way, step, piece):
        di, direction = way
        rows = pl.ds(0, 256) if piece == 0 else pl.ds(256, 272)
        ref = od.at[zed(-direction * (step - 1)), core, rows]
        slot = 2 * step - (2 if piece == di else 1)
        return remote(ref, ref, gz_out.at[di, slot], gz_in.at[di, slot], z_next[di])

    def aside(di, kz):
        ref = ou.at[zed(kz), row, core]
        return remote(ref, ref, uy_out.at[di, kz % NZ], uy_in.at[di, kz % NZ], y_next[di])

    def aside_far(way, kz):
        di, direction = way
        ref = ou.at[zed(kz), why(-direction), core, :, pl.ds(512 * di, 512)]
        return remote(ref, ref, uf_out.at[di, kz % NZ], uf_in.at[di, kz % NZ], y_next[di])

    def across_dn(k):
        ref = od.at[zed(k), core]
        return remote(ref, ref, dpass.at[k % NZ], dgot.at[k % NZ], peer)

    def across_up(ky):
        ref = ou.at[:, why(ky), core]
        return remote(ref, ref, upass.at[ky], ugot.at[ky], peer)

    for way in WAYS:
        go(spread_up(way, 1, way[0]))
        go(spread_up(way, 1, 1 - way[0]))
    for di in (0, 1):
        go(aside(di, 0))

    for copy in tile_copies:
        copy.wait_recv()
    for j in range(5):
        flat = tile_dn[:, :, 128 * j : 128 * j + 128].astype(F32).reshape(128, 128).T.astype(BF16)
        if j < 4:
            od[lay, core, 128 * j : 128 * j + 128] = flat
        else:
            od[lay, core, 512:528] = flat[112:128]
    for way in WAYS:
        go(spread_dn(way, 1, way[0]))
        go(spread_dn(way, 1, 1 - way[0]))
    go(across_dn(0))

    def onward(spread, step):
        for near in (True, False):
            if step == 4 and not near:
                continue
            for way in WAYS:
                piece = way[0] if near else 1 - way[0]
                spread(way, step, piece).wait_recv()
                if step < 3 or (step == 3 and near):
                    go(spread(way, step + 1, piece))

    far = []
    for step in (1, 2, 3, 4):
        onward(spread_up, step)
        for kz in (step, -step) if step < 4 else (4,):
            for di in (0, 1):
                go(aside(di, kz))
        onward(spread_dn, step)
        for k in (step, -step) if step < 4 else (4,):
            go(across_dn(k))
        for kz in (step - 1, 1 - step) if step > 1 else (0,):
            for way in WAYS:
                aside(way[0], kz).wait_recv()
                far.append(go(aside_far(way, kz)))
    go(across_up(0))
    for kz in (4,):
        for way in WAYS:
            aside(way[0], kz).wait_recv()
            far.append(go(aside_far(way, kz)))
    go(across_up(1))
    go(across_up(3))
    for copy in far:
        copy.wait_recv()
    go(across_up(2))

    for k in range(NZ):
        across_dn(k).wait_recv()
    for ky in range(NY):
        across_up(ky).wait_recv()
    for copy in sent:
        copy.wait_send()


def writer(
    ou, od, o_tu, o_td, o_nu, o_nd, o_tn, o_tb, o_nn, o_nb,
    cu, cd, cn, cb, tu, td, tn, tb, nu, nd, nn, nb,
    v_cn, v_cb, sem,
):
    pairs = [(ou, cu)]
    for z in range(NZ):
        for r in (0, 1):
            pairs.append((
                od.at[z, r, pl.ds(0, 512)], cd.at[pl.ds(512 * r, 512), pl.ds(128 * z, 128)]
            ))
    pairs += [
        (o_tu, tu), (o_td, td), (o_nu, nu), (o_nd, nd), (o_tn, tn), (o_tb, tb), (o_nn, nn), (o_nb, nb),
        (v_cn, cn), (v_cb, cb),
    ]
    copies = [pltpu.make_async_copy(a, b, sem.at[i]) for i, (a, b) in enumerate(pairs)]
    for copy in copies[:-2]:
        copy.start()
    for r, line in enumerate((v_cn, v_cb)):
        rows = [od[z, r, 520:528].astype(F32)[7:8] for z in range(NZ)]
        line[...] = jnp.concatenate(rows, axis=0).astype(BF16)
    for copy in copies[-2:]:
        copy.start()
    for copy in copies:
        copy.wait()


def on_device(
    partial_up, partial_down, partial_norm, partial_bias,
    master_up, master_down, master_norm, master_bias,
    memory_up, memory_down, memory_norm, memory_bias,
):
    def shape(s, t=F32):
        return jax.ShapeDtypeStruct(s, t)

    def vm(*s, t=F32):
        return pltpu.VMEM(s, t)

    dma = pltpu.SemaphoreType.DMA
    hbm = pl.BlockSpec(memory_space=pltpu.HBM)
    vmem = pl.BlockSpec(memory_space=pltpu.VMEM)
    made = (
        pltpu.VMEM((NZ, NY, 2, 16, 1024), BF16), pltpu.VMEM((NZ, 2, 528, 128), BF16),
        vm(16, 1024), vm(16, 1024), vm(16, 1024), vm(16, 1024),
        vm(1, 16), vm(1, 16), vm(1, 16), vm(1, 16),
    )
    made = pl.pallas_call(
        kernel,
        out_shape=made,
        in_specs=[hbm] * 12,
        out_specs=(vmem,) * 10,
        scratch_shapes=[
            vm(NY, NZ, 16, 1024), vm(NY, NZ, 16, 1024),
            vm(NZ, 2, 264, 128), vm(NZ, 2, 256, 128), vm(2, 1, 1024), vm(1, 1024),
            vm(2, 3, 4, 16, 1024), vm(2, 7, 264, 128), vm(2, 7, 8, 1024),
            vm(128, 640), vm(2, 3, 16, 640), vm(2, 16, 640),
            vm(2, 16, 640, t=BF16), vm(8, 16, 640, t=BF16),
            vm(16, 1024), vm(16, 1024), vm(16, 1024), vm(16, 1024),
            vm(1, 16), vm(1, 16), vm(1, 16), vm(1, 16),
            dma((NY, 2)), dma((NZ, 2)), dma((10,)), dma((NY, 2)), dma((NZ, 2)), dma,
            dma((NY, 2)), dma((NZ, 2)), dma,
            dma((2, 3)), dma((2, 3)), dma((2, 7)), dma((2, 7)), dma((2, 7)), dma((2, 7)),
            dma((2, 3)), dma((2, 3)), dma, dma,
            dma((NY, 2)), dma((NY, 2)), dma((2, 7)), dma((2, 7)), dma((2, 7)), dma((2, 7)),
            dma((2, NZ)), dma((2, NZ)), dma((2, NZ)), dma((2, NZ)),
            dma((NZ,)), dma((NZ,)), dma((NY,)), dma((NY,)),
        ],
        compiler_params=pltpu.CompilerParams(
            collective_id=0, has_side_effects=True, vmem_limit_bytes=32 * 1024 * 1024
        ),
        name="reduce_step_gather",
    )(*(
        pltpu.with_memory_space_constraint(a, pltpu.HBM)
        for a in (
            partial_up.reshape(NZ, NY, 2, 16, 1024), partial_down[0], partial_norm, partial_bias,
            master_up, master_down.T, master_norm[None], master_bias[None],
            memory_up, memory_down.T, memory_norm[None], memory_bias[None],
        )
    ))
    out = pl.pallas_call(
        writer,
        out_shape=(
            shape((NZ, NY, 2, 16, 1024), BF16), shape((1024, 1024), BF16),
            shape((8, 128), BF16), shape((8, 128), BF16),
            shape((16, 1024)), shape((16, 1024)), shape((1, 16)), shape((1, 16)),
            shape((16, 1024)), shape((16, 1024)), shape((1, 16)), shape((1, 16)),
        ),
        in_specs=[vmem] * 10,
        out_specs=(hbm,) * 12,
        scratch_shapes=[vm(8, 128, t=BF16), vm(8, 128, t=BF16), dma((27,))],
        compiler_params=pltpu.CompilerParams(vmem_limit_bytes=32 * 1024 * 1024),
        name="write_out",
    )(*made)
    cu, cd, cn, cb, tu, td, tn, tb, nu, nd, nn, nb = out
    return (
        cu.reshape(1024, 1024), cd, cn.reshape(1024), cb.reshape(1024),
        tu, td.T, tn[0], tb[0], nu, nd.T, nn[0], nb[0],
    )


def solution(mesh):
    in_specs = (
        P("replica", None, "model"), P("replica", "model", None), P("replica", None), P("replica", None),
        P("replica", "model"), P("model", "replica"), P("replica"), P("replica"),
        P("replica", "model"), P("model", "replica"), P("replica"), P("replica"),
    )
    out_specs = (
        P(None, "model"), P("model", None), P(), P(),
        P("replica", "model"), P("model", "replica"), P("replica"), P("replica"),
        P("replica", "model"), P("model", "replica"), P("replica"), P("replica"),
    )
    return jax.shard_map(
        on_device, mesh=mesh, in_specs=in_specs, out_specs=out_specs, check_vma=False
    )
```

```python
import jax
import jax.numpy as jnp
from jax import lax
from jax.experimental import pallas as pl
from jax.experimental.pallas import tpu as pltpu
from jax.sharding import PartitionSpec as P

learn_rate = 0.05
hold_rate = 0.9
NZ, NY = 8, 4
MEAN_RATE = 64 ** (-0.5)
WAYS = ((0, 1), (1, -1))
F32, BF16 = jnp.float32, jnp.bfloat16


def adapt(total, master, memory):
    mean = total * MEAN_RATE
    state = hold_rate * memory + (1.0 - hold_rate) * mean * mean
    return master - learn_rate * mean * lax.rsqrt(state + 1e-06), state


def wrap(x, most):
    u = jnp.abs(x) * (224.0 / most)
    u2 = u * u
    u4 = u2 * u2
    u8 = u4 * u4
    y = jnp.where(u >= 1.0, u8 * u8, u8)
    return jnp.where(x < 0, -y, y).astype(BF16)


def unwrap(code, most):
    y = code.astype(F32)
    v = jnp.abs(y)
    q = lax.rsqrt(lax.rsqrt(jnp.maximum(v, 1e-37)))
    r8 = q * lax.rsqrt(q)
    r16 = r8 * lax.rsqrt(r8)
    r = jnp.where(v >= 1.0, r16, r8) * (most / 224.0)
    return jnp.where(y > 0, r, jnp.where(y < 0, -r, 0.0))


def slot_of(step, piece, half):
    if step == 1:
        return 0
    return 2 * step - (2 if piece == half else 3)


def kernel(
    up, dn, norm, bias, mu, md, mn, mb, su, sd, sn, sb,
    ou, od, o_tu, o_td, o_nu, o_nd, o_tn, o_tb, o_nn, o_nb,
    own_up, peer_up, own_dn, peer_dn, vecs, peer_vec,
    in_y, in_z, in_z2, to_y, to_z, to_z2, turned, to_yd, in_yd, pair,
    part_dn, tile_dn,
    v_mu, v_md, v_su, v_sd, v_mn, v_mb, v_sn, v_sb,
    load_up, load_dn, load_small, pass_up, pass_dn, pass_vec, got_up, got_dn, got_vec,
    y_out, y_in, z_out, z_in, z2_out, z2_in, yd_out, yd_in,
    tile_out, tile_in, gz_out, gz_in, uz_out, uz_in, uy_out, uy_in, uf_out, uf_in,
    dpass, dgot, upass, ugot,
):
    me = lax.axis_index("replica")
    core = lax.rem(me, 2)
    row = lax.rem(me // 2, NY)
    lay = me // (2 * NY)
    other = 1 - core

    def place(z, y, c):
        return {"replica": (z * NY + y) * 2 + c}

    def zed(k):
        return lax.rem(lay + k + 2 * NZ, NZ)

    def why(k):
        return lax.rem(row + k + 2 * NY, NY)

    peer = place(lay, row, other)
    z_next = [place(zed(way), row, core) for _, way in WAYS]
    y_next = [place(lay, why(way), core) for _, way in WAYS]

    def remote(src, dst, out, arrive, where):
        return pltpu.make_async_remote_copy(
            src_ref=src, dst_ref=dst, send_sem=out, recv_sem=arrive,
            device_id=where, device_id_type=pl.DeviceIdType.MESH,
        )

    sent = []

    def go(copy):
        copy.start()
        sent.append(copy)
        return copy

    smalls = [
        (norm, vecs.at[0]), (bias, vecs.at[1]), (mu, v_mu), (md, v_md), (su, v_su), (sd, v_sd),
        (mn, v_mn), (mb, v_mb), (sn, v_sn), (sb, v_sb),
    ]
    small_copies = [
        pltpu.make_async_copy(a, b, load_small.at[i]) for i, (a, b) in enumerate(smalls)
    ]
    for c in small_copies:
        c.start()

    def up_piece(ky, p, c):
        return up.at[pl.ds(4 * p, 4), why(ky), c]

    def dn_piece(k, p, c):
        rows = pl.multiple_of(c * 512 + p * 256, 256)
        return dn.at[pl.ds(rows, 256), pl.ds(pl.multiple_of(zed(k) * 128, 128), 128)]

    order = [
        ("d", 4, 0), ("d", 4, 1), ("u", 2, 0), ("u", 2, 1), ("d", 3, 1), ("d", 5, 0), ("u", 1, 1), ("u", 3, 0),
        ("d", 3, 0), ("d", 5, 1), ("u", 1, 0), ("u", 3, 1), ("d", 2, 1), ("d", 6, 0), ("d", 2, 0), ("d", 6, 1),
        ("d", 1, 1), ("d", 7, 0), ("d", 1, 0), ("d", 7, 1), ("u", 0, 0), ("u", 0, 1), ("d", 0, 0), ("d", 0, 1),
    ]
    loads, passes = {}, {}
    for kind, k, p in order:
        if kind == "u":
            loads[kind, k, p] = pltpu.make_async_copy(
                up_piece(k, p, core), own_up.at[k, pl.ds(4 * p, 4)], load_up.at[k, p]
            )
            passes[kind, k, p] = remote(
                up_piece(k, p, other), peer_up.at[k, pl.ds(4 * p, 4)],
                pass_up.at[k, p], got_up.at[k, p], peer,
            )
        else:
            loads[kind, k, p] = pltpu.make_async_copy(
                dn_piece(k, p, core), own_dn.at[k, p, pl.ds(0, 256)], load_dn.at[k, p]
            )
            passes[kind, k, p] = remote(
                dn_piece(k, p, other), peer_dn.at[k, p], pass_dn.at[k, p], got_dn.at[k, p], peer
            )

    barrier = pltpu.get_barrier_semaphore()
    friends = [peer] + z_next
    for ky in (1, 2, 3):
        friends += [place(lay, why(ky), core), place(lay, why(ky), other)]
    for friend in friends:
        pl.semaphore_signal(barrier, inc=1, device_id=friend, device_id_type=pl.DeviceIdType.MESH)
    for key in order:
        loads[key].start()
    pl.semaphore_wait(barrier, len(friends))
    small_copies[0].wait()
    small_copies[1].wait()
    vec_pass = go(remote(vecs.at[other], peer_vec, pass_vec, got_vec, peer))
    for key in order:
        go(passes[key])

    vec_pass.wait_recv()
    peer_vec[...] = 0.5 * (vecs[core] + peer_vec[...])

    def join(kind, k, p):
        loads[kind, k, p].wait()
        passes[kind, k, p].wait_recv()
        if kind == "u":
            own_up[k, 4 * p : 4 * p + 4] += peer_up[k, 4 * p : 4 * p + 4]
        else:
            own_dn[k, p, 0:256] += peer_dn[k, p]
            line = peer_vec[:, pl.ds(pl.multiple_of(zed(k) * 128, 128), 128)]
            own_dn[k, p, 256:264] = jnp.broadcast_to(line, (8, 128))

    def reducer(count, mine, leave, arrive, out, inn, neighbour, most):
        reach = count // 2

        def chunk(way, step):
            return (way * (reach + 1 - step)) % count

        def post(way, step, piece, value):
            di = way[0]
            slot = slot_of(step, piece, di)
            leave[di, slot] = wrap(value, most * (step if piece == di else step - 1))
            go(remote(
                leave.at[di, slot], arrive.at[di, slot], out.at[di, slot], inn.at[di, slot], neighbour[di]
            ))

        def send(way, step, piece):
            post(way, step, piece, mine(chunk(way[1], step), piece)[...])

        def take(way, step, piece):
            di, direction = way
            slot = slot_of(step, piece, di)
            remote(
                leave.at[di, slot], arrive.at[di, slot], out.at[di, slot], inn.at[di, slot], neighbour[di]
            ).wait_recv()
            ref = mine(chunk(direction, step + 1), piece)
            total = ref[...] + unwrap(arrive[di, slot], most * (step if piece == di else step - 1))
            if step < reach:
                post(way, step + 1, piece, total)
            else:
                ref[...] = total

        return send, take

    z_send, z_take = reducer(
        NZ, lambda k, p: own_dn.at[k, p], to_z, in_z, z_out, z_in, z_next, 16.0
    )
    y_send, y_take = reducer(
        NY, lambda k, p: own_up.at[k, pl.ds(4 * p, 4)], to_y, in_y, y_out, y_in, y_next, 16.0
    )
    z2_send, z2_take = reducer(
        NZ, lambda k, p: own_up.at[0, zed(k), :, pl.ds(512 * p, 512)],
        to_z2, in_z2, z2_out, z2_in, z_next, 64.0,
    )

    def both(act, step, near):
        for way in WAYS:
            act(way, step, way[0] if near else 1 - way[0])

    def joins(*keys):
        for key in keys:
            join(*key)

    joins(*order[:2])
    both(z_send, 1, True)
    joins(*order[2:4])
    both(y_send, 1, True)
    joins(*order[4:6])
    both(z_send, 2, False)
    joins(*order[6:8])
    both(y_send, 2, False)
    joins(*order[8:10])
    both(z_take, 1, True)
    joins(*order[10:14])
    both(z_take, 2, False)
    both(y_take, 1, True)
    joins(*order[14:18])
    both(z_take, 2, True)
    both(z_take, 3, False)
    joins(*order[18:])
    both(y_take, 2, False)
    both(z_take, 3, True)
    both(y_take, 2, True)
    both(z2_send, 1, True)
    both(z2_send, 2, False)
    both(z_take, 4, False)
    both(z2_take, 1, True)
    both(z_take, 4, True)

    for p in (0, 1):
        turned[:, 256 * p : 256 * p + 256] = own_dn[0, p, 0:256].T
    turned[:, 512:640] = own_dn[0, 0, 136:264].T
    to_yd[...] = wrap(turned[...], 128.0).reshape(8, 16, 640)
    others = [(ky, x) for ky in (2, 1, 3, 0) for x in (0, 1) if (ky, x) != (0, 0)]
    shares = {}
    for ky, x in others:
        c = core if x == 0 else other
        shares[ky, x] = go(remote(
            to_yd.at[2 * why(ky) + c], in_yd.at[core, ky], yd_out.at[ky, x], yd_in.at[ky, x],
            place(lay, why(ky), c),
        ))
    both(z2_take, 2, False)
    both(z2_take, 2, True)
    both(z2_take, 3, False)
    for key in others:
        shares[key].wait_recv()
    pair[core] = turned[pl.ds(pl.multiple_of(16 * (2 * row + core), 16), 16), :] + (
        unwrap(in_yd[core, 1], 128.0) + unwrap(in_yd[core, 2], 128.0) + unwrap(in_yd[core, 3], 128.0)
    )
    pair[other] = (
        unwrap(in_yd[other, 0], 128.0) + unwrap(in_yd[other, 1], 128.0)
        + unwrap(in_yd[other, 2], 128.0) + unwrap(in_yd[other, 3], 128.0)
    )
    for c in small_copies[2:]:
        c.wait()
    lines = ((v_mn, v_sn, o_tn, o_nn), (v_mb, v_sb, o_tb, o_nb))
    for r in (0, 1):
        cols = slice(512 * r, 512 * r + 512)
        stepped, state = adapt(pair[r, :, 0:512], v_md[:, cols], v_sd[:, cols])
        o_td[:, cols] = stepped
        o_nd[:, cols] = state
        part_dn[r, :, 0:512] = stepped.astype(BF16)
        block = jnp.concatenate([pair[r, :, 512:640], jnp.zeros((112, 128), F32)], axis=0).T
        master, memory, o_t, o_n = lines[r]
        stepped, state = adapt(2.0 * block[127:128, 0:16], master[...], memory[...])
        o_t[...] = stepped
        o_n[...] = state
        wide = jnp.concatenate([stepped, jnp.zeros((1, 112), F32)], axis=1)
        part_dn[r, :, 512:640] = jnp.broadcast_to(wide, (128, 128)).T[0:16].astype(BF16)

    tile_copies = []
    for ky in range(NY):
        for x in (0, 1):
            if ky == 0 and x == 0:
                continue
            c = core if x == 0 else other
            tile_copies.append(go(remote(
                part_dn.at[c], tile_dn.at[2 * row + core], tile_out.at[ky, x], tile_in.at[ky, x],
                place(lay, why(ky), c),
            )))
    tile_dn[2 * row + core] = part_dn[core]
    both(z2_take, 3, True)
    both(z2_take, 4, False)
    both(z2_take, 4, True)
    stepped, state = adapt(own_up[0, lay], v_mu[...], v_su[...])
    o_tu[...] = stepped
    o_nu[...] = state
    ou[lay, row, core] = stepped.astype(BF16)

    def spread_up(way, step, piece):
        di, direction = way
        ref = ou.at[zed(-direction * (step - 1)), row, core, :, pl.ds(512 * piece, 512)]
        slot = 2 * step - (2 if piece == di else 1)
        return remote(ref, ref, uz_out.at[di, slot], uz_in.at[di, slot], z_next[di])

    def spread_dn(way, step, piece):
        di, direction = way
        rows = pl.ds(0, 256) if piece == 0 else pl.ds(256, 272)
        ref = od.at[zed(-direction * (step - 1)), core, rows]
        slot = 2 * step - (2 if piece == di else 1)
        return remote(ref, ref, gz_out.at[di, slot], gz_in.at[di, slot], z_next[di])

    def aside(di, kz):
        ref = ou.at[zed(kz), row, core]
        return remote(ref, ref, uy_out.at[di, kz % NZ], uy_in.at[di, kz % NZ], y_next[di])

    def aside_far(way, kz):
        di, direction = way
        ref = ou.at[zed(kz), why(-direction), core, :, pl.ds(512 * di, 512)]
        return remote(ref, ref, uf_out.at[di, kz % NZ], uf_in.at[di, kz % NZ], y_next[di])

    def across_dn(k):
        ref = od.at[zed(k), core]
        return remote(ref, ref, dpass.at[k % NZ], dgot.at[k % NZ], peer)

    def across_up(ky):
        ref = ou.at[:, why(ky), core]
        return remote(ref, ref, upass.at[ky], ugot.at[ky], peer)

    for way in WAYS:
        go(spread_up(way, 1, way[0]))
        go(spread_up(way, 1, 1 - way[0]))
    for di in (0, 1):
        go(aside(di, 0))

    for copy in tile_copies:
        copy.wait_recv()
    for j in range(5):
        flat = tile_dn[:, :, 128 * j : 128 * j + 128].astype(F32).reshape(128, 128).T.astype(BF16)
        if j < 4:
            od[lay, core, 128 * j : 128 * j + 128] = flat
        else:
            od[lay, core, 512:528] = flat[112:128]
    for way in WAYS:
        go(spread_dn(way, 1, way[0]))
        go(spread_dn(way, 1, 1 - way[0]))
    go(across_dn(0))

    def onward(spread, step):
        for near in (True, False):
            if step == 4 and not near:
                continue
            for way in WAYS:
                piece = way[0] if near else 1 - way[0]
                spread(way, step, piece).wait_recv()
                if step < 3 or (step == 3 and near):
                    go(spread(way, step + 1, piece))

    far = []
    for step in (1, 2, 3, 4):
        onward(spread_up, step)
        for kz in (step, -step) if step < 4 else (4,):
            for di in (0, 1):
                go(aside(di, kz))
        onward(spread_dn, step)
        for k in (step, -step) if step < 4 else (4,):
            go(across_dn(k))
        for kz in (step - 1, 1 - step) if step > 1 else (0,):
            for way in WAYS:
                aside(way[0], kz).wait_recv()
                far.append(go(aside_far(way, kz)))
    go(across_up(0))
    for kz in (4,):
        for way in WAYS:
            aside(way[0], kz).wait_recv()
            far.append(go(aside_far(way, kz)))
    go(across_up(1))
    go(across_up(3))
    for copy in far:
        copy.wait_recv()
    go(across_up(2))

    for k in range(NZ):
        across_dn(k).wait_recv()
    for ky in range(NY):
        across_up(ky).wait_recv()
    for copy in sent:
        copy.wait_send()


def writer(
    ou, od, o_tu, o_td, o_nu, o_nd, o_tn, o_tb, o_nn, o_nb,
    cu, cd, cn, cb, tu, td, tn, tb, nu, nd, nn, nb,
    v_cn, v_cb, sem,
):
    pairs = [(ou, cu)]
    for z in range(NZ):
        for r in (0, 1):
            pairs.append((
                od.at[z, r, pl.ds(0, 512)], cd.at[pl.ds(512 * r, 512), pl.ds(128 * z, 128)]
            ))
    pairs += [
        (o_tu, tu), (o_td, td), (o_nu, nu), (o_nd, nd), (o_tn, tn), (o_tb, tb), (o_nn, nn), (o_nb, nb),
        (v_cn, cn), (v_cb, cb),
    ]
    copies = [pltpu.make_async_copy(a, b, sem.at[i]) for i, (a, b) in enumerate(pairs)]
    for copy in copies[:-2]:
        copy.start()
    for r, line in enumerate((v_cn, v_cb)):
        rows = [od[z, r, 520:528].astype(F32)[7:8] for z in range(NZ)]
        line[...] = jnp.concatenate(rows, axis=0).astype(BF16)
    for copy in copies[-2:]:
        copy.start()
    for copy in copies:
        copy.wait()


def on_device(
    partial_up, partial_down, partial_norm, partial_bias,
    master_up, master_down, master_norm, master_bias,
    memory_up, memory_down, memory_norm, memory_bias,
):
    def shape(s, t=F32):
        return jax.ShapeDtypeStruct(s, t)

    def vm(*s, t=F32):
        return pltpu.VMEM(s, t)

    dma = pltpu.SemaphoreType.DMA
    hbm = pl.BlockSpec(memory_space=pltpu.HBM)
    vmem = pl.BlockSpec(memory_space=pltpu.VMEM)
    made = (
        pltpu.VMEM((NZ, NY, 2, 16, 1024), BF16), pltpu.VMEM((NZ, 2, 528, 128), BF16),
        vm(16, 1024), vm(16, 1024), vm(16, 1024), vm(16, 1024),
        vm(1, 16), vm(1, 16), vm(1, 16), vm(1, 16),
    )
    made = pl.pallas_call(
        kernel,
        out_shape=made,
        in_specs=[hbm] * 12,
        out_specs=(vmem,) * 10,
        scratch_shapes=[
            vm(NY, NZ, 16, 1024), vm(NY, NZ, 16, 1024),
            vm(NZ, 2, 264, 128), vm(NZ, 2, 256, 128), vm(2, 1, 1024), vm(1, 1024),
            vm(2, 3, 4, 16, 1024, t=BF16), vm(2, 7, 264, 128, t=BF16), vm(2, 7, 16, 512, t=BF16),
            vm(2, 3, 4, 16, 1024, t=BF16), vm(2, 7, 264, 128, t=BF16), vm(2, 7, 16, 512, t=BF16),
            vm(128, 640), vm(8, 16, 640, t=BF16), vm(2, NY, 16, 640, t=BF16), vm(2, 16, 640),
            vm(2, 16, 640, t=BF16), vm(8, 16, 640, t=BF16),
            vm(16, 1024), vm(16, 1024), vm(16, 1024), vm(16, 1024),
            vm(1, 16), vm(1, 16), vm(1, 16), vm(1, 16),
            dma((NY, 2)), dma((NZ, 2)), dma((10,)), dma((NY, 2)), dma((NZ, 2)), dma,
            dma((NY, 2)), dma((NZ, 2)), dma,
            dma((2, 3)), dma((2, 3)), dma((2, 7)), dma((2, 7)), dma((2, 7)), dma((2, 7)),
            dma((NY, 2)), dma((NY, 2)),
            dma((NY, 2)), dma((NY, 2)), dma((2, 7)), dma((2, 7)), dma((2, 7)), dma((2, 7)),
            dma((2, NZ)), dma((2, NZ)), dma((2, NZ)), dma((2, NZ)),
            dma((NZ,)), dma((NZ,)), dma((NY,)), dma((NY,)),
        ],
        compiler_params=pltpu.CompilerParams(
            collective_id=0, has_side_effects=True, vmem_limit_bytes=32 * 1024 * 1024
        ),
        name="reduce_step_gather",
    )(*(
        pltpu.with_memory_space_constraint(a, pltpu.HBM)
        for a in (
            partial_up.reshape(NZ, NY, 2, 16, 1024), partial_down[0], partial_norm, partial_bias,
            master_up, master_down.T, master_norm[None], master_bias[None],
            memory_up, memory_down.T, memory_norm[None], memory_bias[None],
        )
    ))
    out = pl.pallas_call(
        writer,
        out_shape=(
            shape((NZ, NY, 2, 16, 1024), BF16), shape((1024, 1024), BF16),
            shape((8, 128), BF16), shape((8, 128), BF16),
            shape((16, 1024)), shape((16, 1024)), shape((1, 16)), shape((1, 16)),
            shape((16, 1024)), shape((16, 1024)), shape((1, 16)), shape((1, 16)),
        ),
        in_specs=[vmem] * 10,
        out_specs=(hbm,) * 12,
        scratch_shapes=[vm(8, 128, t=BF16), vm(8, 128, t=BF16), dma((27,))],
        compiler_params=pltpu.CompilerParams(vmem_limit_bytes=32 * 1024 * 1024),
        name="write_out",
    )(*made)
    cu, cd, cn, cb, tu, td, tn, tb, nu, nd, nn, nb = out
    return (
        cu.reshape(1024, 1024), cd, cn.reshape(1024), cb.reshape(1024),
        tu, td.T, tn[0], tb[0], nu, nd.T, nn[0], nb[0],
    )


def solution(mesh):
    in_specs = (
        P("replica", None, "model"), P("replica", "model", None), P("replica", None), P("replica", None),
        P("replica", "model"), P("model", "replica"), P("replica"), P("replica"),
        P("replica", "model"), P("model", "replica"), P("replica"), P("replica"),
    )
    out_specs = (
        P(None, "model"), P("model", None), P(), P(),
        P("replica", "model"), P("model", "replica"), P("replica"), P("replica"),
        P("replica", "model"), P("model", "replica"), P("replica"), P("replica"),
    )
    return jax.shard_map(
        on_device, mesh=mesh, in_specs=in_specs, out_specs=out_specs, check_vma=False
    )
```

```python
import jax
import jax.numpy as jnp
from jax import lax
from jax.experimental import pallas as pl
from jax.experimental.pallas import tpu as pltpu
from jax.sharding import PartitionSpec as P

learn_rate = 0.05
hold_rate = 0.9
NZ, NY = 8, 4
MEAN_RATE = 64 ** (-0.5)
WAYS = ((0, 1), (1, -1))
F32, BF16 = jnp.float32, jnp.bfloat16


def adapt(total, master, memory):
    mean = total * MEAN_RATE
    state = hold_rate * memory + (1.0 - hold_rate) * mean * mean
    return master - learn_rate * mean * lax.rsqrt(state + 1e-06), state


def wrap(x, most):
    u = jnp.abs(x) * (224.0 / most)
    u2 = u * u
    u4 = u2 * u2
    u8 = u4 * u4
    y = jnp.where(u >= 1.0, u8 * u8, u8)
    return jnp.where(x < 0, -y, y).astype(BF16)


def unwrap(code, most):
    y = code.astype(F32)
    v = jnp.abs(y)
    q = lax.rsqrt(lax.rsqrt(jnp.maximum(v, 1e-37)))
    r8 = q * lax.rsqrt(q)
    r16 = r8 * lax.rsqrt(r8)
    r = jnp.where(v >= 1.0, r16, r8) * (most / 224.0)
    return jnp.where(y > 0, r, jnp.where(y < 0, -r, 0.0))


def slot_of(step, piece, half):
    if step == 1:
        return 0
    return 2 * step - (2 if piece == half else 3)


def kernel(
    up, dn, norm, bias, mu, md, mn, mb, su, sd, sn, sb,
    ou, od, o_tu, o_td, o_nu, o_nd, o_tn, o_tb, o_nn, o_nb,
    own_up, peer_up, own_dn, peer_dn, vecs, peer_vec,
    in_y, in_z, in_z2, to_y, to_z, to_z2, turned, to_yd, in_yd, pair,
    part_dn, tile_dn,
    v_mu, v_md, v_su, v_sd, v_mn, v_mb, v_sn, v_sb,
    join_in, vec_in, small_in, vec_out, join_out,
    y_in, z_in, z2_in, yd_in, tile_in, gz_in, uz_in, uy_in, uf_in, dgot, ugot,
    y_out, z_out, z2_out, yd_out, tile_out, gz_out, uz_out, uy_out, uf_out, dpass, upass,
):
    me = lax.axis_index("replica")
    core = lax.rem(me, 2)
    row = lax.rem(me // 2, NY)
    lay = me // (2 * NY)
    other = 1 - core

    def place(z, y, c):
        return {"replica": (z * NY + y) * 2 + c}

    def zed(k):
        return lax.rem(lay + k + 2 * NZ, NZ)

    def why(k):
        return lax.rem(row + k + 2 * NY, NY)

    peer = place(lay, row, other)
    z_next = [place(zed(way), row, core) for _, way in WAYS]
    y_next = [place(lay, why(way), core) for _, way in WAYS]

    def remote(src, dst, out, arrive, where):
        return pltpu.make_async_remote_copy(
            src_ref=src, dst_ref=dst, send_sem=out, recv_sem=arrive,
            device_id=where, device_id_type=pl.DeviceIdType.MESH,
        )

    def go(copy):
        copy.start()
        return copy

    def settle(ref, sem):
        pltpu.make_async_copy(ref, ref, sem).wait()

    smalls = [
        (norm, vecs.at[0]), (bias, vecs.at[1]), (mu, v_mu), (md, v_md), (su, v_su), (sd, v_sd),
        (mn, v_mn), (mb, v_mb), (sn, v_sn), (sb, v_sb),
    ]
    where = (0, 0, 1, 1, 1, 1, 2, 3, 4, 5)
    small_copies = [
        pltpu.make_async_copy(a, b, small_in.at[i]) for i, (a, b) in zip(where, smalls)
    ]
    for c in small_copies:
        c.start()

    def up_piece(ky, p, c):
        return up.at[pl.ds(4 * p, 4), why(ky), c]

    def dn_piece(k, p, c):
        rows = pl.multiple_of(c * 512 + p * 256, 256)
        return dn.at[pl.ds(rows, 256), pl.ds(pl.multiple_of(zed(k) * 128, 128), 128)]

    order = [
        ("d", 4, 0), ("d", 4, 1), ("u", 2, 0), ("u", 2, 1), ("d", 3, 1), ("d", 5, 0), ("d", 3, 0), ("d", 5, 1),
        ("u", 1, 1), ("u", 3, 0), ("u", 1, 0), ("u", 3, 1), ("d", 2, 1), ("d", 6, 0), ("d", 2, 0), ("d", 6, 1),
        ("d", 1, 1), ("d", 7, 0), ("d", 1, 0), ("d", 7, 1), ("u", 0, 0), ("u", 0, 1), ("d", 0, 0), ("d", 0, 1),
    ]
    loads, passes = [], []
    for i, (kind, k, p) in enumerate(order):
        sem = join_in.at[i // 2]
        if kind == "u":
            loads.append(pltpu.make_async_copy(
                up_piece(k, p, core), own_up.at[k, pl.ds(4 * p, 4)], sem
            ))
            passes.append(remote(
                up_piece(k, p, other), peer_up.at[k, pl.ds(4 * p, 4)], join_out.at[0], sem, peer
            ))
        else:
            loads.append(pltpu.make_async_copy(dn_piece(k, p, core), own_dn.at[k, p, pl.ds(0, 256)], sem))
            passes.append(remote(dn_piece(k, p, other), peer_dn.at[k, p], join_out.at[1], sem, peer))

    barrier = pltpu.get_barrier_semaphore()
    friends = [peer] + z_next
    for ky in (1, 2, 3):
        friends += [place(lay, why(ky), core), place(lay, why(ky), other)]
    for friend in friends:
        pl.semaphore_signal(barrier, inc=1, device_id=friend, device_id_type=pl.DeviceIdType.MESH)
    for copy in loads:
        copy.start()
    pl.semaphore_wait(barrier, len(friends))
    settle(vecs, small_in.at[0])
    vec_pass = go(remote(vecs.at[other], peer_vec, vec_out, vec_in, peer))
    for copy in passes:
        go(copy)

    vec_pass.wait_recv()
    peer_vec[...] = 0.5 * (vecs[core] + peer_vec[...])

    def join(i):
        pair_of = order[2 * i : 2 * i + 2]
        settle((peer_up if pair_of[0][0] == "u" else peer_dn).at[pl.ds(0, 2)], join_in.at[i])
        for kind, k, p in pair_of:
            if kind == "u":
                own_up[k, 4 * p : 4 * p + 4] += peer_up[k, 4 * p : 4 * p + 4]
            else:
                own_dn[k, p, 0:256] += peer_dn[k, p]
                line = peer_vec[:, pl.ds(pl.multiple_of(zed(k) * 128, 128), 128)]
                own_dn[k, p, 256:264] = jnp.broadcast_to(line, (8, 128))

    def reducer(count, mine, leave, arrive, out, inn, neighbour, most):
        reach = count // 2

        def chunk(way, step):
            return (way * (reach + 1 - step)) % count

        def copy_of(way, step, piece):
            di = way[0]
            slot = slot_of(step, piece, di)
            return remote(leave.at[di, slot], arrive.at[di, slot], out, inn.at[di, slot], neighbour[di])

        def post(way, step, piece, value):
            di = way[0]
            leave[di, slot_of(step, piece, di)] = wrap(value, most * (step if piece == di else step - 1))
            go(copy_of(way, step, piece))

        def send(way, step, piece):
            post(way, step, piece, mine(chunk(way[1], step), piece)[...])

        def take(way, step, piece):
            di, direction = way
            copy_of(way, step, piece).wait_recv()
            ref = mine(chunk(direction, step + 1), piece)
            sofar = most * (step if piece == di else step - 1)
            total = ref[...] + unwrap(arrive[di, slot_of(step, piece, di)], sofar)
            if step < reach:
                post(way, step + 1, piece, total)
            else:
                ref[...] = total

        return send, take

    z_send, z_take = reducer(
        NZ, lambda k, p: own_dn.at[k, p], to_z, in_z, z_out, z_in, z_next, 16.0
    )
    y_send, y_take = reducer(
        NY, lambda k, p: own_up.at[k, pl.ds(4 * p, 4)], to_y, in_y, y_out, y_in, y_next, 16.0
    )
    z2_send, z2_take = reducer(
        NZ, lambda k, p: own_up.at[0, zed(k), :, pl.ds(512 * p, 512)],
        to_z2, in_z2, z2_out, z2_in, z_next, 64.0,
    )

    def both(act, step, near):
        for way in WAYS:
            act(way, step, way[0] if near else 1 - way[0])

    join(0)
    both(z_send, 1, True)
    join(1)
    both(y_send, 1, True)
    join(2)
    both(z_send, 2, False)
    join(3)
    join(4)
    both(z_take, 1, True)
    both(y_send, 2, False)
    join(5)
    join(6)
    both(z_take, 2, False)
    join(7)
    both(y_take, 1, True)
    both(z_take, 2, True)
    join(8)
    both(z_take, 3, False)
    join(9)
    join(10)
    both(y_take, 2, False)
    both(z_take, 3, True)
    join(11)
    both(y_take, 2, True)
    both(z2_send, 1, True)
    both(z_take, 4, False)
    both(z2_send, 2, False)
    both(z_take, 4, True)

    for p in (0, 1):
        turned[:, 256 * p : 256 * p + 256] = own_dn[0, p, 0:256].T
    turned[:, 512:640] = own_dn[0, 0, 136:264].T
    to_yd[...] = wrap(turned[...], 128.0).reshape(8, 16, 640)
    others = [(ky, x) for ky in (2, 1, 3, 0) for x in (0, 1) if (ky, x) != (0, 0)]
    for ky, x in others:
        c = core if x == 0 else other
        go(remote(
            to_yd.at[2 * why(ky) + c], in_yd.at[NY * core + ky], yd_out, yd_in, place(lay, why(ky), c)
        ))
    settle(own_up.at[1, pl.ds(0, 4)], small_in.at[1])
    for i in range(2, 6):
        small_copies[4 + i].wait()
    both(z2_take, 1, True)
    both(z2_take, 2, False)
    both(z2_take, 2, True)
    settle(in_yd.at[pl.ds(1, 7)], yd_in)

    def came(c, ky):
        return unwrap(in_yd[NY * c + ky], 128.0)

    pair[core] = turned[pl.ds(pl.multiple_of(16 * (2 * row + core), 16), 16), :] + (
        came(core, 1) + came(core, 2) + came(core, 3)
    )
    pair[other] = came(other, 0) + came(other, 1) + came(other, 2) + came(other, 3)
    lines = ((v_mn, v_sn, o_tn, o_nn), (v_mb, v_sb, o_tb, o_nb))
    for r in (0, 1):
        cols = slice(512 * r, 512 * r + 512)
        stepped, state = adapt(pair[r, :, 0:512], v_md[:, cols], v_sd[:, cols])
        o_td[:, cols] = stepped
        o_nd[:, cols] = state
        part_dn[r, :, 0:512] = stepped.astype(BF16)
        block = jnp.concatenate([pair[r, :, 512:640], jnp.zeros((112, 128), F32)], axis=0).T
        master, memory, o_t, o_n = lines[r]
        stepped, state = adapt(2.0 * block[127:128, 0:16], master[...], memory[...])
        o_t[...] = stepped
        o_n[...] = state
        wide = jnp.concatenate([stepped, jnp.zeros((1, 112), F32)], axis=1)
        part_dn[r, :, 512:640] = jnp.broadcast_to(wide, (128, 128)).T[0:16].astype(BF16)

    for ky, x in others:
        c = core if x == 0 else other
        go(remote(
            part_dn.at[c], tile_dn.at[2 * row + core], tile_out, tile_in, place(lay, why(ky), c)
        ))
    tile_dn[2 * row + core] = part_dn[core]

    both(z2_take, 3, False)
    both(z2_take, 3, True)
    both(z2_take, 4, False)
    both(z2_take, 4, True)
    stepped, state = adapt(own_up[0, lay], v_mu[...], v_su[...])
    o_tu[...] = stepped
    o_nu[...] = state
    ou[lay, row, core] = stepped.astype(BF16)

    def spread_up(way, step, piece):
        di, direction = way
        ref = ou.at[zed(-direction * (step - 1)), row, core, :, pl.ds(512 * piece, 512)]
        slot = 2 * step - (2 if piece == di else 1)
        return remote(ref, ref, uz_out, uz_in.at[di, slot], z_next[di])

    def aside(di, kz):
        ref = ou.at[zed(kz), row, core]
        return remote(ref, ref, uy_out, uy_in.at[kz % NZ], y_next[di])

    def aside_far(way, kz):
        di, direction = way
        ref = ou.at[zed(kz), why(-direction), core, :, pl.ds(512 * di, 512)]
        return remote(ref, ref, uf_out, uf_in.at[kz % NZ], y_next[di])

    def across_up(kz, ky):
        ref = ou.at[zed(kz), why(ky), core]
        return remote(ref, ref, upass, ugot, peer)

    def share(kz):
        for di in (0, 1):
            go(aside(di, kz))
        go(across_up(kz, 0))

    def turn(kz):
        settle(ou.at[0, pl.ds(0, 2), 0], uy_in.at[kz % NZ])
        for way in WAYS:
            go(aside_far(way, kz))
        for way in WAYS:
            go(across_up(kz, -way[1]))

    def turned_far(kz):
        settle(ou.at[0, 0, 0], uf_in.at[kz % NZ])
        go(across_up(kz, 2))

    def spread_dn(way, step, piece):
        di, direction = way
        rows = pl.ds(0, 256) if piece == 0 else pl.ds(256, 272)
        ref = od.at[zed(-direction * (step - 1)), core, rows]
        slot = 2 * step - (2 if piece == di else 1)
        return remote(ref, ref, gz_out, gz_in.at[di, slot], z_next[di])

    def across_dn(k):
        ref = od.at[zed(k), core]
        return remote(ref, ref, dpass, dgot, peer)

    def onward(spread, step, near):
        for way in WAYS:
            piece = way[0] if near else 1 - way[0]
            spread(way, step, piece).wait_recv()
            if step < 3 or (step == 3 and near):
                go(spread(way, step + 1, piece))

    def up_step(step):
        onward(spread_up, step, True)
        if step < 4:
            onward(spread_up, step, False)
            share(step)
        share(-step) if step < 4 else share(4)

    for near in (True, False):
        for way in WAYS:
            go(spread_up(way, 1, way[0] if near else 1 - way[0]))
    share(0)
    settle(tile_dn.at[pl.ds(0, 7)], tile_in)
    for j in range(5):
        flat = tile_dn[:, :, 128 * j : 128 * j + 128].astype(F32).reshape(128, 128).T.astype(BF16)
        if j < 4:
            od[lay, core, 128 * j : 128 * j + 128] = flat
        else:
            od[lay, core, 512:528] = flat[112:128]
    for way in WAYS:
        go(spread_dn(way, 1, way[0]))
    go(across_dn(0))
    up_step(1)
    for way in WAYS:
        go(spread_dn(way, 1, 1 - way[0]))
    up_step(2)
    onward(spread_dn, 1, True)
    turn(0)
    onward(spread_dn, 1, False)
    go(across_dn(1))
    go(across_dn(-1))
    up_step(3)
    turn(1)
    turn(-1)
    onward(spread_dn, 2, True)
    turned_far(0)
    up_step(4)
    onward(spread_dn, 2, False)
    go(across_dn(2))
    go(across_dn(-2))
    turn(2)
    turn(-2)
    turned_far(1)
    turned_far(-1)
    onward(spread_dn, 3, True)
    turn(3)
    turn(-3)
    turned_far(2)
    turned_far(-2)
    turn(4)
    onward(spread_dn, 3, False)
    go(across_dn(3))
    go(across_dn(-3))
    turned_far(3)
    turned_far(-3)
    turned_far(4)
    onward(spread_dn, 4, True)
    go(across_dn(4))

    settle(peer_vec, vec_out)
    settle(peer_up, join_out.at[0])
    settle(peer_dn, join_out.at[1])
    settle(to_y, y_out)
    settle(to_z, z_out)
    settle(to_z2, z2_out)
    settle(to_yd.at[pl.ds(0, 7)], yd_out)
    settle(tile_dn.at[pl.ds(0, 7)], tile_out)
    settle(od.at[pl.ds(0, 7), 0], gz_out)
    settle(to_z2, uz_out)
    settle(ou.at[:, pl.ds(0, 2), 0], uy_out)
    settle(ou.at[:, 0, 0], uf_out)
    settle(ou.at[:, :, 0], upass)
    settle(od.at[:, 0], dpass)
    settle(ou.at[:, :, other], ugot)
    settle(od.at[:, other], dgot)


def writer(
    ou, od, o_tu, o_td, o_nu, o_nd, o_tn, o_tb, o_nn, o_nb,
    cu, cd, cn, cb, tu, td, tn, tb, nu, nd, nn, nb,
    v_cn, v_cb, sem,
):
    pairs = [(ou, cu)]
    for z in range(NZ):
        for r in (0, 1):
            pairs.append((
                od.at[z, r, pl.ds(0, 512)], cd.at[pl.ds(512 * r, 512), pl.ds(128 * z, 128)]
            ))
    pairs += [
        (o_tu, tu), (o_td, td), (o_nu, nu), (o_nd, nd), (o_tn, tn), (o_tb, tb), (o_nn, nn), (o_nb, nb),
        (v_cn, cn), (v_cb, cb),
    ]
    copies = [pltpu.make_async_copy(a, b, sem.at[i]) for i, (a, b) in enumerate(pairs)]
    for copy in copies[:-2]:
        copy.start()
    for r, line in enumerate((v_cn, v_cb)):
        rows = [od[z, r, 520:528].astype(F32)[7:8] for z in range(NZ)]
        line[...] = jnp.concatenate(rows, axis=0).astype(BF16)
    for copy in copies[-2:]:
        copy.start()
    for copy in copies:
        copy.wait()


def on_device(
    partial_up, partial_down, partial_norm, partial_bias,
    master_up, master_down, master_norm, master_bias,
    memory_up, memory_down, memory_norm, memory_bias,
):
    def shape(s, t=F32):
        return jax.ShapeDtypeStruct(s, t)

    def vm(*s, t=F32):
        return pltpu.VMEM(s, t)

    dma = pltpu.SemaphoreType.DMA
    hbm = pl.BlockSpec(memory_space=pltpu.HBM)
    vmem = pl.BlockSpec(memory_space=pltpu.VMEM)
    made = (
        pltpu.VMEM((NZ, NY, 2, 16, 1024), BF16), pltpu.VMEM((NZ, 2, 528, 128), BF16),
        vm(16, 1024), vm(16, 1024), vm(16, 1024), vm(16, 1024),
        vm(1, 16), vm(1, 16), vm(1, 16), vm(1, 16),
    )
    made = pl.pallas_call(
        kernel,
        out_shape=made,
        in_specs=[hbm] * 12,
        out_specs=(vmem,) * 10,
        scratch_shapes=[
            vm(NY, NZ, 16, 1024), vm(NY, NZ, 16, 1024),
            vm(NZ, 2, 264, 128), vm(NZ, 2, 256, 128), vm(2, 1, 1024), vm(1, 1024),
            vm(2, 3, 4, 16, 1024, t=BF16), vm(2, 7, 264, 128, t=BF16), vm(2, 7, 16, 512, t=BF16),
            vm(2, 3, 4, 16, 1024, t=BF16), vm(2, 7, 264, 128, t=BF16), vm(2, 7, 16, 512, t=BF16),
            vm(128, 640), vm(8, 16, 640, t=BF16), vm(2 * NY, 16, 640, t=BF16), vm(2, 16, 640),
            vm(2, 16, 640, t=BF16), vm(8, 16, 640, t=BF16),
            vm(16, 1024), vm(16, 1024), vm(16, 1024), vm(16, 1024),
            vm(1, 16), vm(1, 16), vm(1, 16), vm(1, 16),
            dma((12,)), dma, dma((6,)), dma, dma((2,)),
            dma((2, 3)), dma((2, 7)), dma((2, 7)), dma, dma, dma((2, 7)), dma((2, 7)), dma((NZ,)), dma((NZ,)), dma, dma,
            dma, dma, dma, dma, dma, dma, dma, dma, dma, dma, dma,
        ],
        compiler_params=pltpu.CompilerParams(
            collective_id=0, has_side_effects=True, vmem_limit_bytes=32 * 1024 * 1024
        ),
        name="reduce_step_gather",
    )(*(
        pltpu.with_memory_space_constraint(a, pltpu.HBM)
        for a in (
            partial_up.reshape(NZ, NY, 2, 16, 1024), partial_down[0], partial_norm, partial_bias,
            master_up, master_down.T, master_norm[None], master_bias[None],
            memory_up, memory_down.T, memory_norm[None], memory_bias[None],
        )
    ))
    out = pl.pallas_call(
        writer,
        out_shape=(
            shape((NZ, NY, 2, 16, 1024), BF16), shape((1024, 1024), BF16),
            shape((8, 128), BF16), shape((8, 128), BF16),
            shape((16, 1024)), shape((16, 1024)), shape((1, 16)), shape((1, 16)),
            shape((16, 1024)), shape((16, 1024)), shape((1, 16)), shape((1, 16)),
        ),
        in_specs=[vmem] * 10,
        out_specs=(hbm,) * 12,
        scratch_shapes=[vm(8, 128, t=BF16), vm(8, 128, t=BF16), dma((27,))],
        compiler_params=pltpu.CompilerParams(vmem_limit_bytes=32 * 1024 * 1024),
        name="write_out",
    )(*made)
    cu, cd, cn, cb, tu, td, tn, tb, nu, nd, nn, nb = out
    return (
        cu.reshape(1024, 1024), cd, cn.reshape(1024), cb.reshape(1024),
        tu, td.T, tn[0], tb[0], nu, nd.T, nn[0], nb[0],
    )


def solution(mesh):
    in_specs = (
        P("replica", None, "model"), P("replica", "model", None), P("replica", None), P("replica", None),
        P("replica", "model"), P("model", "replica"), P("replica"), P("replica"),
        P("replica", "model"), P("model", "replica"), P("replica"), P("replica"),
    )
    out_specs = (
        P(None, "model"), P("model", None), P(), P(),
        P("replica", "model"), P("model", "replica"), P("replica"), P("replica"),
        P("replica", "model"), P("model", "replica"), P("replica"), P("replica"),
    )
    return jax.shard_map(
        on_device, mesh=mesh, in_specs=in_specs, out_specs=out_specs, check_vma=False
    )
```
